256 devices in a mesh: pb: 2 (over y), band: 128 (over z, x, core).
Axes of the slice: x: 4, y: 2, z: 16, core: 2. Of those that a mesh axis runs over, the one named last changes fastest.
The devices are a block of a 4x16x16 slice.
Arguments:
- wavefunctions: bfloat16 [2, 64, 16384], P(None, None, 'band'), may hold values from -6 to 6
- k_vectors: float32 [3, 16384], P(None, 'band'), may hold values from -2 to 2
- beta_k: bfloat16 [2, 16384, 3072], P(None, 'band'), may hold values from -0.03125 to 0.03125
- beta_kq: bfloat16 [2, 32768, 3072], P(None, ('pb', 'band')), parts along dimension 1, may hold values from -0.078125 to 0.078125
- kq_vectors: float32 [3, 32768], P(None, ('pb', 'band')), parts along dimension 1, may hold values from -2 to 2
- d_matrix: float32 [4, 8, 8], replicated, may hold values from -2.1 to 2.1
- species: int32 [384], replicated, may hold values from 0 to 3
- displacements: float32 [6, 384, 3], P('pb'), parts along dimension 0, may hold values from -6 to 6
Outputs:
- response: bfloat16 [6, 2, 64, 16384], P('pb', None, None, 'band'), parts along dimension 0
The draws below stay inside these ranges and needn't reach their ends.
There are 2 independent parts, one for each index of `pb`. The reference program is written for one: setup_inputs(seed, part) draws one part's arguments, and reference() takes and returns one part's arrays. A program takes and returns all parts, laid end to end along the dimension named above; an argument that names none is the same for every part. Nothing has to cross between parts.
All inputs are finite; a program needn't handle non-finite values.
Results may differ from the reference program's by a relative error of at most 0.0054.
Values sent between devices are 32-bit elements; how exact they have to be, the bound alone decides.
A program may use at most 128 MiB of HBM per device.

```python
import jax
import jax.numpy as jnp
from jax import lax

NB = 64
NH = 8
NSP = 4
NPW = 16384
NAT = 384
P_SIZE = 3072


def with_ends(array, own_key, smallest, high):
    dims = array.shape
    spot = [jax.random.randint(jax.random.fold_in(own_key, axis), (), 0, dims[axis]) for axis in range(len(dims))]
    array = array.at[tuple(spot)].set(smallest)
    longest = dims.index(max(dims))
    spot[longest] = (spot[longest] + 1) % dims[longest]
    return array.at[tuple(spot)].set(high)


def steps_of(rng, dims, split, least, top_value):
    loudness = 1.0
    for axis_at, shards_of in split:
        steps = jax.random.uniform(jax.random.fold_in(jax.random.fold_in(rng, 6), axis_at), (shards_of,), jnp.float32, least / len(split), top_value / len(split))
        loudness = loudness * jnp.repeat(jnp.exp(steps), dims[axis_at] // shards_of).reshape((-1,) + (1,) * (len(dims) - 1 - axis_at))
    return loudness


def scatter_about(own_key, shape, spread, limit, cuts=(), kind=jnp.bfloat16):
    result = jax.random.normal(own_key, shape, jnp.float32) * spread
    if len(cuts) > 0:
        result = steps_of(own_key, shape, cuts, -0.22, 0.18) * result
    return jnp.clip(result, min=-limit, max=limit).astype(kind)


def setup_inputs(seed: int = 0, part: int = 0) -> dict:
    seeds = jax.random.split(jax.random.key(seed), 9)
    own_keys = jax.random.split(jax.random.fold_in(seeds[8], part), 9)
    return {
        "wavefunctions": scatter_about(seeds[0], (2, NB, NPW), 1.0, 6.0, ((2, 128),)),
        "k_vectors": jnp.clip(jax.random.uniform(seeds[1], (3, NPW), jnp.float32, -2.0, 2.0) * steps_of(seeds[1], (3, NPW), ((1, 128),), -0.4, 0.0), -2.0, 2.0),
        "beta_k": scatter_about(seeds[2], (2, NPW, P_SIZE), (2 * NPW) ** -0.5, 0.03125, ((1, 128),)),
        "beta_kq": scatter_about(own_keys[3], (2, NPW, P_SIZE), (2 * P_SIZE) ** -0.5, 0.078125, ((1, 128),)),
        "kq_vectors": jnp.clip(jax.random.uniform(own_keys[4], (3, NPW), jnp.float32, -2.0, 2.0) * steps_of(own_keys[4], (3, NPW), ((1, 128),), -0.4, 0.0), -2.0, 2.0),
        "d_matrix": scatter_about(seeds[5], (NSP, NH, NH), 0.35, 2.1, (), jnp.float32),
        "species": with_ends(jax.random.randint(seeds[6], (NAT,), 0, NSP), jax.random.fold_in(seeds[6], 1), 0, NSP - 1).astype(jnp.int32),
        "displacements": scatter_about(own_keys[7], (3, NAT, 3), 1.0, 6.0, (), jnp.float32),
    }


def scaled_columns(waves, k_vectors):
    waves_f = waves.astype(jnp.float32)
    moved = waves_f[:, None, :, :] * k_vectors[None, :, None, :]
    stacked = jnp.concatenate([waves_f[:, None], moved], axis=1).astype(jnp.bfloat16)
    band_count = waves.shape[1]
    wave_count = waves.shape[2]
    real_part = stacked[0].reshape(4 * band_count, wave_count)
    imag_part = stacked[1].reshape(4 * band_count, wave_count)
    return jnp.stack([jnp.concatenate([real_part, imag_part], 0), jnp.concatenate([imag_part, -real_part], 0)])


def atom_matrices(species, d_matrix):
    kinds = jnp.arange(d_matrix.shape[0], dtype=jnp.int32)
    onehot = (species[:, None] == kinds[None, :]).astype(jnp.float32)
    per_atom = d_matrix.shape[1]
    flat = jnp.dot(onehot, d_matrix.reshape(d_matrix.shape[0], per_atom * per_atom), precision=lax.Precision.HIGHEST)
    return flat.reshape(species.shape[0], per_atom, per_atom)


def apply_dmat(block, atom_mats):
    shaped = block.reshape(atom_mats.shape[0], atom_mats.shape[1], block.shape[1])
    mixed = jnp.einsum("aij,ajc->aic", atom_mats, shaped, precision=lax.Precision.HIGHEST)
    return mixed.reshape(block.shape)


def coefficients(dcols, modes_part, per_atom):
    row_count = dcols.shape[0]
    band_count = dcols.shape[1] // 8
    pieces = dcols.reshape(row_count, 2, 4, band_count)
    weights = jnp.repeat(modes_part, per_atom, axis=1)
    turned_real = jnp.einsum("mpa,pab->mpb", weights, pieces[:, 0, 1:], precision=lax.Precision.HIGHEST)
    turned_imag = jnp.einsum("mpa,pab->mpb", weights, pieces[:, 1, 1:], precision=lax.Precision.HIGHEST)
    plain_real = weights[:, :, :, None] * pieces[None, :, 0, 0][:, :, None, :]
    plain_imag = weights[:, :, :, None] * pieces[None, :, 1, 0][:, :, None, :]
    real_part = jnp.concatenate([-turned_imag[:, :, None], plain_real], axis=2)
    imag_part = jnp.concatenate([turned_real[:, :, None], plain_imag], axis=2)
    real_part = real_part.transpose(1, 0, 2, 3).reshape(row_count, 12 * band_count).astype(jnp.bfloat16)
    imag_part = imag_part.transpose(1, 0, 2, 3).reshape(row_count, 12 * band_count).astype(jnp.bfloat16)
    return jnp.stack([jnp.concatenate([real_part, imag_part], 1), jnp.concatenate([-imag_part, real_part], 1)])


def project_back(coef, beta_cols):
    return lax.dot_general(coef, beta_cols, (((0, 1), (0, 2)), ((), ())), preferred_element_type=jnp.float32)


def finish(back, kq_vectors, band_count):
    pieces = back.reshape(2, 3, 4, band_count, back.shape[1])
    back_real = pieces[0]
    back_imag = pieces[1]
    shifted = kq_vectors[None, :, None, :]
    out_real = back_real[:, 0] + jnp.sum(shifted * back_imag[:, 1:], axis=1)
    out_imag = back_imag[:, 0] - jnp.sum(shifted * back_real[:, 1:], axis=1)
    return jnp.stack([out_real, out_imag], 1).astype(jnp.bfloat16)


def reference(wavefunctions, k_vectors, beta_k, beta_kq, kq_vectors, d_matrix, species, displacements):
    right = scaled_columns(wavefunctions, k_vectors)
    becp = lax.dot_general(beta_k, right, (((0, 1), (0, 2)), ((), ())), preferred_element_type=jnp.float32)
    dcols = apply_dmat(becp, atom_matrices(species, d_matrix))
    coef = coefficients(dcols, displacements, d_matrix.shape[1])
    back = project_back(coef, beta_kq)
    return finish(back, kq_vectors, wavefunctions.shape[1])
```

```python
import functools

import jax
import jax.numpy as jnp
from jax import lax
from jax.experimental import pallas as pl
from jax.experimental.pallas import tpu as pltpu
from jax.sharding import PartitionSpec as P

CORES = 2
X = 4
SLOTS = 3
LANES = 128
SEMS = 320


def kernel(
    Z,
    waves,
    kvec,
    beta_k,
    beta_kq_hbm,
    kq,
    dtile,
    sp,
    w,
    out,
    left,
    W,
    CR,
    XA,
    XB,
    ZA,
    ZB,
    G,
    C,
    bkq,
    kq_sem,
    ssem,
    rsem,
):
    half = Z // 2
    me = lax.axis_index("band")
    pb = lax.axis_index("pb")
    c = lax.rem(me, CORES)
    x = lax.rem(lax.div(me, CORES), X)
    z = lax.div(me, CORES * X)
    h = lax.rem(pb, 2)

    def xat(d):
        return lax.rem(x + (X + d), X)

    def zat(d):
        return lax.rem(z + (Z + d), Z)

    def dev(zz, xx, cc):
        return {"band": (zz * X + xx) * CORES + cc}

    other = dev(z, x, 1 - c)
    xr, xl = dev(z, xat(1), c), dev(z, xat(-1), c)
    zr, zl = dev(zat(1), x, c), dev(zat(-1), x, c)
    pair = {"pb": pb + 1 - 2 * h}

    load_kq = pltpu.make_async_copy(beta_kq_hbm, bkq, kq_sem)
    load_kq.start()

    barrier = pltpu.get_barrier_semaphore()
    for who in (other, xr, xl, zr, zl, pair):
        pl.semaphore_signal(barrier, inc=1, device_id=who, device_id_type=pl.DeviceIdType.MESH)

    ids = {}
    pending = []

    def number(key):
        return ids.setdefault(key, len(ids))

    def describe(key, src, dst, who):
        at = number(key)
        return pltpu.make_async_remote_copy(
            src_ref=src,
            dst_ref=dst,
            send_sem=ssem.at[at],
            recv_sem=rsem.at[at],
            device_id=who,
            device_id_type=pl.DeviceIdType.MESH,
        )

    def send(key, src, dst, who):
        copy = describe(key, src, dst, who)
        copy.start()
        pending.append(copy)

    def receive(key, land, who):
        describe(key, land, land, who).wait_recv()

    sre = waves[0].astype(jnp.float32)
    sim = waves[1].astype(jnp.float32)
    bands = sre.shape[0]
    for s in range(4):
        row = 1.0 if s == 0 else kvec[s - 1 : s, :]
        a_part = sre * row
        b_part = sim * row
        rows = pl.ds(s * bands, bands)
        left[rows, 0:LANES] = jnp.where(h == 0, a_part, b_part).astype(jnp.bfloat16)
        left[rows, LANES : 2 * LANES] = jnp.where(h == 0, b_part, -a_part).astype(jnp.bfloat16)

    def product(cc, s, two):
        lanes = pl.multiple_of((cc * SLOTS * X + s * X + two * 2) * LANES, 2 * LANES)
        right = beta_k[:, :, pl.ds(lanes, 2 * LANES)].reshape(2 * LANES, 2 * LANES)
        value = jnp.dot(left[...], right, preferred_element_type=jnp.float32)
        for k in range(2):
            part = value[:, k * LANES : (k + 1) * LANES]
            W[cc, s, 2 * two + k] = part.reshape(W.shape[3:])

    for s in range(SLOTS):
        for two in range(2):
            product(1 - c, s, two)
            if s == 0 and two == 0:
                pl.semaphore_wait(barrier, 6)
            here = pl.ds(2 * two, 2)
            send(("core", s, two), W.at[1 - c, s, here], CR.at[s, here], other)
    for s in range(SLOTS):
        for two in range(2):
            product(c, s, two)

    def x_start(tag, a, b, buf):
        send((tag, 0), a(xat(2)), buf.at[0], xr)
        send((tag, 1), b(xat(2)), buf.at[1], xl)
        send((tag, 2), b(xat(1)), buf.at[2], xr)
        send((tag, 3), a(xat(-1)), buf.at[3], xl)

    def x_middle(tag, a, b, buf):
        receive((tag, 0), buf.at[0], xl)
        a(xat(1))[...] += buf[0]
        send((tag, 4), a(xat(1)), buf.at[4], xr)
        receive((tag, 1), buf.at[1], xr)
        b(xat(-1))[...] += buf[1]
        send((tag, 5), b(xat(-1)), buf.at[5], xl)

    def x_last(tag, a, b, buf):
        receive((tag, 2), buf.at[2], xl)
        receive((tag, 3), buf.at[3], xr)
        receive((tag, 4), buf.at[4], xl)
        receive((tag, 5), buf.at[5], xr)
        a(x)[...] += buf[3] + buf[4]
        b(x)[...] += buf[2] + buf[5]

    def z_send(tag, chunk, buf, k):
        if k < half:
            send((tag, 0, k), chunk(zat(half - k)), buf.at[k], zr)
        if k < half - 1:
            send((tag, 1, k), chunk(zat(k + 1 - half)), buf.at[half + k], zl)

    def z_step(tag, chunk, buf, k):
        if k < half:
            receive((tag, 0, k), buf.at[k], zl)
            chunk(zat(half - 1 - k))[...] += buf[k]
            if k + 1 < half:
                send((tag, 0, k + 1), chunk(zat(half - k - 1)), buf.at[k + 1], zr)
        if k < half - 1:
            receive((tag, 1, k), buf.at[half + k], zr)
            chunk(zat(k + 2 - half))[...] += buf[half + k]
            if k + 1 < half - 1:
                send((tag, 1, k + 1), chunk(zat(k + 2 - half)), buf.at[half + k + 1], zl)

    def a0(t):
        return W.at[c, 0, t, pl.ds(0, half)]

    def b0(t):
        return W.at[c, 0, t, pl.ds(half, half)]

    def a12(t):
        return W.at[c, 1, t, z]

    def b12(t):
        return W.at[c, 2, t, z]

    def chunk0(t):
        return W.at[c, 0, x, t]

    def chunk_of(s):
        return lambda t: W.at[c, s, pl.ds(0, X), t]

    for s in range(SLOTS):
        for two in range(2):
            here = pl.ds(2 * two, 2)
            receive(("core", s, two), CR.at[s, here], other)
            W[c, s, here] += CR[s, here]
        if s == 0:
            x_start("x0", a0, b0, XA)
        else:
            z_send(("z", s), chunk_of(s), ZB.at[s - 1], 0)

    row_atom = lax.broadcasted_iota(jnp.int32, (LANES, LANES), 0) // 8
    lane_atom = lax.broadcasted_iota(jnp.int32, (LANES, LANES), 1) // 8
    same = row_atom == lane_atom

    def mixer(s):
        kinds = sp[pl.ds((c * SLOTS + s) * X + x, 1), :]
        total = jnp.zeros((LANES, LANES), jnp.float32)
        for kind in range(dtile.shape[0]):
            total = jnp.where(same & (kinds == kind), dtile[kind], total)
        return total

    for i in range(half + 3):
        if i < half:
            for s in (1, 2):
                z_step(("z", s), chunk_of(s), ZB.at[s - 1], i)
        if i == 1:
            x_middle("x0", a0, b0, XA)
        if i == 2:
            x_last("x0", a0, b0, XA)
            z_send(("z", 0), chunk0, ZA, 0)
        if i >= 3:
            z_step(("z", 0), chunk0, ZA, i - 3)
        if i == half:
            x_start("x12", a12, b12, XB)
        if i == half + 1:
            x_middle("x12", a12, b12, XB)
        if i == half + 2:
            x_last("x12", a12, b12, XB)

    for s in range(SLOTS):
        G[h, c, s, x, z] = jnp.dot(
            W[c, s, x, z],
            mixer(s),
            precision=lax.Precision.HIGHEST,
            preferred_element_type=jnp.float32,
        )

    both = pl.ds(0, 2)
    three = pl.ds(0, SLOTS)
    four = pl.ds(0, X)
    mine = G.at[h, c, three, x, z]
    send("pair", mine, mine, pair)
    theirs = G.at[1 - h, c, three, x, z]
    receive("pair", theirs, pair)

    def slot_chunk(s):
        return lambda t: G.at[both, c, s, x, t]

    def group_chunk(hh):
        return lambda t: G.at[hh, c, 2, four, t]

    def g_send(tag, chunk, k):
        if k < half:
            send((tag, 0, k), chunk(zat(-k)), chunk(zat(-k)), zr)
        if k < half - 1:
            send((tag, 1, k), chunk(zat(k)), chunk(zat(k)), zl)

    def g_step(tag, chunk, k):
        if k < half:
            land = chunk(zat(-1 - k))
            receive((tag, 0, k), land, zl)
            if k + 1 < half:
                send((tag, 0, k + 1), land, land, zr)
        if k < half - 1:
            land = chunk(zat(k + 1))
            receive((tag, 1, k), land, zr)
            if k + 1 < half - 1:
                send((tag, 1, k + 1), land, land, zl)

    def gx_start(tag, view):
        send((tag, 0), view(both, x), view(both, x), xr)
        send((tag, 1), view(both, x), view(both, x), xl)

    def gx_middle(tag, view):
        receive((tag, 0), view(both, xat(-1)), xl)
        send((tag, 2), view(pl.ds(0, 1), xat(-1)), view(pl.ds(0, 1), xat(-1)), xr)
        receive((tag, 1), view(both, xat(1)), xr)
        send((tag, 3), view(pl.ds(1, 1), xat(1)), view(pl.ds(1, 1), xat(1)), xl)

    def gx_last(tag, view):
        receive((tag, 2), view(pl.ds(0, 1), xat(2)), xl)
        receive((tag, 3), view(pl.ds(1, 1), xat(2)), xr)

    def view01(zz):
        return lambda hh, t: G.at[hh, c, pl.ds(0, 2), t, zz]

    def view2(hh, t):
        return G.at[hh, c, 2, t, z]

    def reached(k):
        if k < 0:
            return [(0, z)]
        found = []
        if k < half:
            found.append((-1 - k, zat(-1 - k)))
        if k < half - 1:
            found.append((k + 1, zat(k + 1)))
        return found

    def to_core(k):
        for d, zz in reached(k):
            block = G.at[both, c, three, four, zz]
            send(("other", d), block, block, other)

    for s in (0, 1):
        g_send(("g", s), slot_chunk(s), 0)
    gx_start("gx2", view2)
    gx_start(("gx", 0), view01(z))
    gx_middle("gx2", view2)
    for i in range(half + 2):
        if i < half:
            for s in (0, 1):
                g_step(("g", s), slot_chunk(s), i)
        if i == 0:
            gx_last("gx2", view2)
            for hh in range(2):
                g_send(("h", hh), group_chunk(hh), 0)
        if i >= 2:
            for hh in range(2):
                g_step(("h", hh), group_chunk(hh), i - 2)
        if i < half:
            for d, zz in reached(i):
                gx_start(("gx", d), view01(zz))
        if i <= half:
            for d, zz in reached(i - 1):
                gx_middle(("gx", d), view01(zz))
        if i >= 1:
            for d, zz in reached(i - 2):
                gx_last(("gx", d), view01(zz))
            to_core(i - 2)
    for k in range(-1, half):
        for d, zz in reached(k):
            receive(("other", d), G.at[both, 1 - c, three, four, zz], other)

    per = bands // (Z // 4)

    def coefficients(n, carry):
        nc = lax.div(n, SLOTS * X)
        ns = lax.rem(lax.div(n, X), SLOTS)
        nx = lax.rem(n, X)
        lanes = pl.ds(pl.multiple_of(n * LANES, LANES), LANES)
        for j in range(Z // 4):
            re = [G[0, nc, ns, nx, s * (Z // 4) + j] for s in range(4)]
            im = [G[1, nc, ns, nx, s * (Z // 4) + j] for s in range(4)]
            for m in range(w.shape[0] // 3):
                ws = [w[3 * m + a : 3 * m + a + 1, lanes] for a in range(3)]
                turned_re = -(ws[0] * im[1] + ws[1] * im[2] + ws[2] * im[3])
                turned_im = ws[0] * re[1] + ws[1] * re[2] + ws[2] * re[3]
                real = [turned_re] + [ws[a] * re[0] for a in range(3)]
                imag = [turned_im] + [ws[a] * im[0] for a in range(3)]
                for t in range(4):
                    at = (m * 8 + t) * bands + j * per
                    C[at : at + per, lanes] = real[t].astype(jnp.bfloat16)
                    at += 4 * bands
                    C[at : at + per, lanes] = imag[t].astype(jnp.bfloat16)
        return carry

    lax.fori_loop(0, CORES * SLOTS * X, coefficients, 0)
    load_kq.wait()

    def back(m, carry):
        rows = pl.ds(pl.multiple_of(m * 8 * bands, 8 * bands), 8 * bands)
        right = bkq[...].reshape(2 * LANES, bkq.shape[2])
        both_parts = lax.dot_general(
            C[rows, :], right, (((1,), (1,)), ((), ())), preferred_element_type=jnp.float32
        )
        top = both_parts[: 4 * bands]
        low = both_parts[4 * bands :]
        back_re = top[:, :LANES] - low[:, LANES:]
        back_im = top[:, LANES:] + low[:, :LANES]
        out_re = back_re[:bands]
        out_im = back_im[:bands]
        for a in range(3):
            rows_a = slice((1 + a) * bands, (2 + a) * bands)
            out_re = out_re + kq[a : a + 1, :] * back_im[rows_a]
            out_im = out_im - kq[a : a + 1, :] * back_re[rows_a]
        out[m, 0] = out_re.astype(jnp.bfloat16)
        out[m, 1] = out_im.astype(jnp.bfloat16)
        return carry

    lax.fori_loop(0, out.shape[0], back, 0)
    for copy in pending:
        copy.wait_send()


def solution(mesh):
    Z = mesh.shape["band"] // (CORES * X)

    def body(waves, kvec, beta_k, beta_kq, kq, d_matrix, species, displacements):
        bands = waves.shape[1]
        projectors = beta_k.shape[2]
        modes = displacements.shape[0]
        per_atom = d_matrix.shape[1]
        per = 4 * bands // Z
        dtile = jnp.tile(d_matrix.transpose(0, 2, 1), (1, LANES // per_atom, LANES // per_atom))
        sp = jnp.repeat(species, per_atom).reshape(projectors // LANES, LANES)
        w = jnp.repeat(displacements.transpose(0, 2, 1).reshape(modes * 3, -1), per_atom, axis=1)
        vmem = pl.BlockSpec(memory_space=pltpu.VMEM)
        f32 = jnp.float32
        return pl.pallas_call(
            functools.partial(kernel, Z),
            out_shape=jax.ShapeDtypeStruct((modes, 2, bands, beta_kq.shape[1]), jnp.bfloat16),
            in_specs=[vmem, vmem, vmem, pl.BlockSpec(memory_space=pl.ANY), vmem, vmem, vmem, vmem],
            out_specs=vmem,
            scratch_shapes=[
                pltpu.VMEM((4 * bands, 2 * LANES), jnp.bfloat16),
                pltpu.VMEM((CORES, SLOTS, X, Z, per, LANES), f32),
                pltpu.VMEM((SLOTS, X, Z, per, LANES), f32),
                pltpu.VMEM((6, Z // 2, per, LANES), f32),
                pltpu.VMEM((6, per, LANES), f32),
                pltpu.VMEM((Z, per, LANES), f32),
                pltpu.VMEM((2, Z, X, per, LANES), f32),
                pltpu.VMEM((2, CORES, SLOTS, X, Z, per, LANES), f32),
                pltpu.VMEM((modes * 8 * bands, projectors), jnp.bfloat16),
                pltpu.VMEM(beta_kq.shape, jnp.bfloat16),
                pltpu.SemaphoreType.DMA,
                pltpu.SemaphoreType.DMA((SEMS,)),
                pltpu.SemaphoreType.DMA((SEMS,)),
            ],
            compiler_params=pltpu.CompilerParams(
                collective_id=0, has_side_effects=True, vmem_limit_bytes=56 * 2**20
            ),
        )(waves, kvec, beta_k, beta_kq, kq, dtile, sp, w)

    in_specs = (
        P(None, None, "band"),
        P(None, "band"),
        P(None, "band", None),
        P(None, ("pb", "band"), None),
        P(None, ("pb", "band")),
        P(),
        P(),
        P("pb", None, None),
    )
    out_specs = P("pb", None, None, "band")
    return jax.shard_map(body, mesh=mesh, in_specs=in_specs, out_specs=out_specs, check_vma=False)
```
